32 devices in a mesh: px: 8 (over z, y), py: 4 (over x, core).
Axes of the slice: x: 2, y: 2, z: 4, core: 2. Of those that a mesh axis runs over, the one named last changes fastest.
Arguments:
- mode_field: float32 [64, 512, 1024], P(None, 'px', 'py'), may hold values from -1 to 1
- forcing: float32 [64, 512, 1024], P(None, 'px', 'py'), may hold values from -8 to 8
- visc_base: float32 [64, 1024, 512], P('py', 'px'), may hold values from 0.1 to 3
- depth_inverse: float32 [1024, 64, 64], P('py'), may hold values from -1 to 2, as said below
Outputs:
- mode_field_out: float32 [64, 512, 1024], P(None, 'px', 'py')
- residual_norms: float32 [2], replicated
The draws below stay inside these ranges and needn't reach their ends.
Inputs may be any that keep to these rules, and one draw needn't show every extreme that they name: `depth_inverse`: each matrix has its diagonal between 0.5 and 1.5 and off-diagonal entries of magnitude at most 0.4 / sqrt(64).
All inputs are finite; a program needn't handle non-finite values.
Results may differ from the reference program's by a relative error of at most 0.0001.
Values sent between devices are 32-bit elements; how exact they have to be, the bound alone decides.
A program may use at most 128 MiB of HBM per device.

```python
import math
import jax
import jax.numpy as jnp
from jax import lax

Z = 64
NX = 1024
NY = 512
ITERS = 2


def draw_depth_inverse(key, part):
    first = jax.random.fold_in(key, 11)
    second = jax.random.fold_in(key, 12)
    spread = 0.4 / math.sqrt(Z)
    offdiag = jax.random.uniform(first, (NX, Z, Z), jnp.float32, -spread, spread)
    diagonal = jax.random.uniform(second, (NX, Z), jnp.float32, 0.5, 1.5)
    identity = jnp.eye(Z, dtype=jnp.float32)
    return offdiag * (1.0 - identity) + diagonal[:, :, None] * identity


def block_levels(stream_key, dims, shards, low, largest):
    loudness = 1.0
    for axis_at, parts in shards:
        steps = jax.random.uniform(jax.random.fold_in(jax.random.fold_in(stream_key, 6), axis_at), (parts,), jnp.float32, low / len(shards), largest / len(shards))
        loudness = loudness * jnp.repeat(jnp.exp(steps), dims[axis_at] // parts).reshape((-1,) + (1,) * (len(dims) - 1 - axis_at))
    return loudness


def gaussian(key, extent, deviation, reach, cuts=(), kind=jnp.bfloat16):
    result = jax.random.normal(key, extent, jnp.float32) * deviation
    if len(cuts) > 0:
        result = block_levels(key, extent, cuts, -0.22, 0.18) * result
    return jnp.clip(result, min=-reach, max=reach).astype(kind)


def setup_inputs(seed: int = 0) -> dict:
    splits = jax.random.split(jax.random.key(seed), 5)
    return {
        "mode_field": gaussian(splits[0], (Z, NY, NX), 0.125, 1.0, ((1, 8), (2, 4)), jnp.float32),
        "forcing": gaussian(splits[1], (Z, NY, NX), 1.0, 8.0, ((1, 8), (2, 4)), jnp.float32),
        "visc_base": jnp.clip(jnp.exp(math.log(3.0) - 3.4011974 * jax.random.uniform(splits[2], (Z, NX, NY), jnp.float32) ** block_levels(splits[2], (Z, NX, NY), ((0, 4), (1, 8)), -0.2, 0.2)), 0.1, 3.0),
        "depth_inverse": draw_depth_inverse(jax.random.fold_in(splits[4], 71), 0),
    }


def depth_tables(count):
    index = jnp.arange(count, dtype=jnp.float32)
    angle = jnp.pi * index[:, None] * index[None, :] / (count - 1)
    ends = jnp.where((index == 0) | (index == count - 1), 2.0, 1.0)
    forward = jnp.cos(angle)
    backward = 2.0 / (count - 1) * jnp.cos(angle) / (ends[:, None] * ends[None, :])
    return (forward, backward)

def hartley_axis(values, axis):
    spectrum = jnp.fft.fft(values, axis=axis)
    return (jnp.real(spectrum) - jnp.imag(spectrum)) / math.sqrt(values.shape[axis])

def wavenumber(count):
    index = jnp.arange(count, dtype=jnp.int32)
    folded = jnp.minimum(index, count - index).astype(jnp.float32)
    scaled = 2.0 * jnp.pi * folded / count
    return scaled * scaled

def reference(mode_field, forcing, visc_base, depth_inverse):
    forward, backward = depth_tables(Z)
    lateral = wavenumber(NY)[:, None] + wavenumber(NX)[None, :]
    field = mode_field
    norms = []
    for sweep in range(ITERS):
        points = jnp.einsum('jm,myx->jyx', forward, field, precision=lax.Precision.HIGHEST)
        physical = jnp.transpose(hartley_axis(hartley_axis(points, 2), 1), (0, 2, 1))
        stress = visc_base * jnp.power(1.0 + physical * physical, -1.0 / 3.0) * physical
        spectral = hartley_axis(hartley_axis(jnp.transpose(stress, (0, 2, 1)), 1), 2)
        viscous = jnp.einsum('mj,jyx->myx', backward, spectral, precision=lax.Precision.HIGHEST)
        residual = forcing - (lateral * field + viscous)
        norms.append(jnp.mean(residual * residual))
        correction = jnp.einsum('xmn,nyx->myx', depth_inverse, residual, precision=lax.Precision.HIGHEST)
        field = field + correction / (1.0 + lateral)
    return (field, jnp.stack(norms))
```

```python
import functools
import math

import jax
import jax.numpy as jnp
from jax import lax
from jax.experimental import pallas as pl
from jax.experimental.pallas import tpu as pltpu
from jax.sharding import PartitionSpec as P

ITERS = 2
MESH = pl.DeviceIdType.MESH
HIGH = lax.Precision.HIGH
VMEM_LIMIT = 60000 * 1024


def depth_tables(count):
    index = jnp.arange(count, dtype=jnp.float32)
    angle = jnp.pi * index[:, None] * index[None, :] / (count - 1)
    ends = jnp.where((index == 0) | (index == count - 1), 2.0, 1.0)
    forward = jnp.cos(angle)
    backward = 2.0 / (count - 1) * jnp.cos(angle) / (ends[:, None] * ends[None, :])
    return (forward, backward)


def hartley_table(count):
    index = jnp.arange(count, dtype=jnp.int32)
    phase = index[:, None] * index[None, :] % count
    angle = phase.astype(jnp.float32) * (2.0 * math.pi / count)
    return (jnp.cos(angle) + jnp.sin(angle)) / math.sqrt(count)


def wave_square(index, count):
    folded = jnp.minimum(index, count - index).astype(jnp.float32)
    scaled = 2.0 * jnp.pi * folded / count
    return scaled * scaled


def part(axis, size, index):
    if axis == 0:
        return (pl.ds(index * size, size),)
    start = pl.multiple_of(index * size, 128 if axis == 2 else 8)
    return (slice(None),) * axis + (pl.ds(start, size),)


def exchange_kernel(name, count, split, concat, x_ref, o_ref, own_sem, send_sems, recv_sems):
    me = lax.axis_index(name)
    split_size = x_ref.shape[split] // count
    concat_size = x_ref.shape[concat]
    barrier = pltpu.get_barrier_semaphore()
    for step in range(1, count):
        peer = lax.rem(me + step, count)
        pl.semaphore_signal(barrier, inc=1, device_id={name: peer}, device_id_type=MESH)
    pl.semaphore_wait(barrier, count - 1)
    copies = []
    for step in range(1, count):
        peer = lax.rem(me + step, count)
        copy = pltpu.make_async_remote_copy(
            src_ref=x_ref.at[part(split, split_size, peer)],
            dst_ref=o_ref.at[part(concat, concat_size, me)],
            send_sem=send_sems.at[step - 1],
            recv_sem=recv_sems.at[step - 1],
            device_id={name: peer},
            device_id_type=MESH,
        )
        copy.start()
        copies.append(copy)
    own = pltpu.make_async_copy(
        x_ref.at[part(split, split_size, me)], o_ref.at[part(concat, concat_size, me)], own_sem
    )
    own.start()
    own.wait()
    for copy in copies:
        copy.wait()


def exchange(x, name, split, concat, ident):
    count = lax.axis_size(name)
    split_size = x.shape[split] // count
    concat_size = x.shape[concat]
    units = (1, 8, 128)
    if split_size % units[split] or concat_size % units[concat]:
        return lax.all_to_all(x, name, split_axis=split, concat_axis=concat, tiled=True)
    shape = list(x.shape)
    shape[split] = split_size
    shape[concat] = concat_size * count
    return pl.pallas_call(
        functools.partial(exchange_kernel, name, count, split, concat),
        out_shape=jax.ShapeDtypeStruct(tuple(shape), x.dtype),
        in_specs=[pl.BlockSpec(memory_space=pl.ANY)],
        out_specs=pl.BlockSpec(memory_space=pl.ANY),
        scratch_shapes=[
            pltpu.SemaphoreType.DMA,
            pltpu.SemaphoreType.DMA((count - 1,)),
            pltpu.SemaphoreType.DMA((count - 1,)),
        ],
        compiler_params=pltpu.CompilerParams(collective_id=ident, has_side_effects=True),
        name="exchange_" + name + str(ident),
    )(x)


def table_halves(x):
    high = lax.reduce_precision(x, 8, 7)
    return high.astype(jnp.bfloat16), (x - high).astype(jnp.bfloat16)


def halves(x):
    high = x.astype(jnp.bfloat16)
    low = (x - high.astype(jnp.float32)).astype(jnp.bfloat16)
    return high, low


def dot3(a, b, dims=(((1,), (0,)), ((), ()))):
    a_high, a_low = a
    b_high, b_low = b
    dot = functools.partial(lax.dot_general, dimension_numbers=dims, preferred_element_type=jnp.float32)
    return dot(a_high, b_high) + (dot(a_high, b_low) + dot(a_low, b_high))


def lateral_kernel(group, high_ref, low_ref, columns_ref, visc_ref, out_ref):
    table = (high_ref[...], low_ref[...])
    columns = jnp.concatenate([columns_ref[i] for i in range(group)], axis=1)
    physical = dot3(table, halves(columns))
    visc = jnp.concatenate([visc_ref[i].T for i in range(group)], axis=1)
    stress = visc * jnp.exp(jnp.log(1.0 + physical * physical) * (-1.0 / 3.0)) * physical
    back = dot3(table, halves(stress))
    width = back.shape[1] // group
    for i in range(group):
        out_ref[i] = back[:, i * width:(i + 1) * width]


def lateral_stage(table, columns, visc_base):
    depth, total_y, cells_x = columns.shape
    group = 2 if depth % 2 == 0 and cells_x % 128 == 0 else 1
    return pl.pallas_call(
        functools.partial(lateral_kernel, group),
        grid=(depth // group,),
        out_shape=jax.ShapeDtypeStruct(columns.shape, columns.dtype),
        in_specs=[
            pl.BlockSpec((total_y, total_y), lambda z: (0, 0)),
            pl.BlockSpec((total_y, total_y), lambda z: (0, 0)),
            pl.BlockSpec((group, total_y, cells_x), lambda z: (z, 0, 0)),
            pl.BlockSpec((group, cells_x, total_y), lambda z: (z, 0, 0)),
        ],
        out_specs=pl.BlockSpec((group, total_y, cells_x), lambda z: (z, 0, 0)),
        compiler_params=pltpu.CompilerParams(vmem_limit_bytes=VMEM_LIMIT),
        name="lateral_stage",
    )(*table, columns, visc_base)


def lines_kernel(high_ref, low_ref, x_ref, out_ref):
    out_ref[...] = dot3(halves(x_ref[...]), (high_ref[...], low_ref[...]))


def lines_stage(table, x):
    depth, rows, total = x.shape
    flat = x.reshape(depth * rows, total)
    tile = math.gcd(depth * rows, 256)
    out = pl.pallas_call(
        lines_kernel,
        grid=(depth * rows // tile,),
        out_shape=jax.ShapeDtypeStruct(flat.shape, flat.dtype),
        in_specs=[
            pl.BlockSpec((total, total), lambda i: (0, 0)),
            pl.BlockSpec((total, total), lambda i: (0, 0)),
            pl.BlockSpec((tile, total), lambda i: (i, 0)),
        ],
        out_specs=pl.BlockSpec((tile, total), lambda i: (i, 0)),
        compiler_params=pltpu.CompilerParams(vmem_limit_bytes=VMEM_LIMIT),
        name="lines_stage",
    )(*table, flat)
    return out.reshape(x.shape)


def local(mode_field, forcing, visc_base, depth_inverse):
    depth_count = mode_field.shape[0]
    rows_y = mode_field.shape[1]
    cols_x = mode_field.shape[2]
    total_y = rows_y * lax.axis_size("px")
    total_x = cols_x * lax.axis_size("py")
    cell_total = depth_count * total_y * total_x
    forward, backward = depth_tables(depth_count)
    table_x = table_halves(hartley_table(total_x))
    table_y = table_halves(hartley_table(total_y))
    index_y = lax.axis_index("px") * rows_y + jnp.arange(rows_y, dtype=jnp.int32)
    index_x = lax.axis_index("py") * cols_x + jnp.arange(cols_x, dtype=jnp.int32)
    lateral = wave_square(index_y, total_y)[:, None] + wave_square(index_x, total_x)[None, :]
    field = mode_field
    partials = []
    for sweep in range(ITERS):
        points = jnp.einsum("jm,myx->jyx", forward, field, precision=HIGH)
        lines = exchange(points, "py", 0, 2, 0)
        lines = lines_stage(table_x, lines)
        columns = exchange(lines, "px", 2, 1, 1)
        returned = lateral_stage(table_y, columns, visc_base)
        returned = exchange(returned, "px", 1, 2, 2)
        returned = lines_stage(table_x, returned)
        spectral = exchange(returned, "py", 2, 0, 3)
        viscous = jnp.einsum("mj,jyx->myx", backward, spectral, precision=HIGH)
        residual = forcing - (lateral * field + viscous)
        squares = jnp.sum(residual * residual)
        partials.append(squares)
        correction = jnp.einsum("xmn,nyx->myx", depth_inverse, residual, precision=HIGH)
        field = field + correction / (1.0 + lateral)
    norm_values = lax.psum(jnp.stack(partials), ("px", "py")) / cell_total
    return (field, norm_values)


def solution(mesh):
    placed = (P(None, "px", "py"), P(None, "px", "py"), P("py", "px", None), P("py", None, None))
    return jax.shard_map(
        local, mesh=mesh, in_specs=placed, out_specs=(P(None, "px", "py"), P()), check_vma=False
    )
```
